32 devices in a mesh: section: 4 (over z), expert: 4 (over y, core), seq: 2 (over x).
Axes of the slice: x: 2, y: 2, z: 4, core: 2. Of those that a mesh axis runs over, the one named last changes fastest.
Arguments:
- tokens: bfloat16 [512, 4096], P('expert', 'section'), may hold values from -6 to 6
- route_ids: int32 [512, 2], P('expert'), may hold values from 0 to 3, all different within a row; in each aligned block of 128 rows (0 to 127, 128 to 255, ...) at most 96 rows name the same one
- route_weights: float32 [512, 2], P('expert'), may hold values from 0.25 to 1
- gate_weight: bfloat16 [4, 4096, 8192], P('expert', None, ('section', 'seq')), may hold values from -0.09375 to 0.09375
- up_weight: bfloat16 [4, 4096, 8192], P('expert', None, ('section', 'seq')), may hold values from -0.09375 to 0.09375
- down_weight: bfloat16 [4, 8192, 4096], P('expert', 'section', 'seq'), may hold values from -0.0625 to 0.0625
Outputs:
- mixed: bfloat16 [512, 4096], P('expert', 'seq')
The draws below stay inside these ranges and needn't reach their ends.
Inputs may be any that keep to these rules, and one draw needn't show every extreme that they name: `route_ids`: the two ids of a token differ; among the 128 tokens of one source group (held on one index of the expert axis) no expert is named more than 96 times.
All inputs are finite; a program needn't handle non-finite values.
Results may differ from the reference program's by a relative error of at most 0.0057.
Values may be sent and summed in bfloat16 or wider, within the bound.
A program may use at most 64 MiB of HBM per device.

```python
import math
import jax
import jax.numpy as jnp
import numpy as np
from jax import lax

D = 4096
FF = 8192
TOP = 2
TOK = 128
EXPERTS = 4
CAP = 96
TOKENS = 512


def steps_of(own_key, extent, split, least, top_value):
    loudness, own = 1.0, jax.random.fold_in(own_key, 6)
    for dim, shards_of in split:
        draws = jnp.exp(jax.random.uniform(jax.random.fold_in(own, dim), (shards_of,), jnp.float32, least / len(split), top_value / len(split)))
        loudness = loudness * jnp.repeat(draws, extent[dim] // shards_of).reshape([-1 if axis == dim else 1 for axis in range(len(extent))])
    return loudness


def routed_block(stream_key, own, number, rows, amount, top, reach, slope):
    order = jax.random.permutation(stream_key, amount)
    packed, common = shares(amount, rows * top, reach, slope, True), shares(amount, rows * top, reach, slope, False)
    places = jnp.arange(amount)

    def named(lengths, turn):
        used = int((lengths > 0).sum())
        fixed = max(1, used // 4)
        passed = fixed + (places - fixed + turn * (used - fixed)) % max(1, amount - fixed)
        return jnp.zeros((amount,), jnp.int32).at[order[jnp.where(places < fixed, places, passed)]].set(jnp.asarray(lengths, jnp.int32))

    lengths = jnp.where(number % 4 == 0, named(packed, number // 4), named(common, number - number // 4 - 1))
    mixed = jax.random.permutation(jax.random.fold_in(own, 3), amount)
    donor, taker = mixed[0:amount // 2 * 2:2], mixed[1:amount // 2 * 2:2]
    room = jnp.minimum(lengths[donor] - 1, reach - lengths[taker]) // 2
    room = jnp.where((donor == order[0]) | (taker == order[0]) | (lengths[taker] == 0), 0, jnp.maximum(room, 0))
    passed = jax.random.randint(jax.random.fold_in(own, 4), (amount // 2,), 0, 1 << 20) % (room + 1)
    lengths = lengths.at[donor].add(-passed).at[taker].add(passed)
    items = jnp.searchsorted(jnp.cumsum(lengths), jnp.arange(rows * top), side="right").astype(jnp.int32)
    listing = items.reshape(top, rows).T
    listing = listing[jax.random.permutation(jax.random.fold_in(own, 1), rows)]
    turn = jax.random.randint(jax.random.fold_in(own, 2), (rows, 1), 0, top)
    return jnp.take_along_axis(listing, (jnp.arange(top)[None, :] + turn) % top, axis=1)


def shares(count, total, most, lean, full):
    loads = [(1 << 20) // math.isqrt(standing ** lean) + 1 for standing in range(1, count + 1)]
    largest = most if full else min(most, max(-(-total // count), total * loads[0] // sum(loads)))
    least = 1 if total - largest >= count - 1 else 0
    given, spare = [largest] + [least] * (count - 1), total - largest - least * (count - 1)
    while spare > 0:
        movable = [i for i in range(1, count) if given[i] < largest] or [i for i in range(1, count) if given[i] < most]
        pool, budget = sum([loads[i] for i in movable]), spare
        for i in movable:
            addition = min(most - given[i], max(1, budget * loads[i] // pool), spare)
            given[i] = given[i] + addition
            spare = spare - addition
    return np.array(given)


def gaussian(own_key, extent, width, reach, pieces=(), kind=jnp.bfloat16):
    factor_of = steps_of(own_key, extent, pieces, -0.22, 0.18) if pieces else 1.0
    array = jax.random.normal(own_key, extent, jnp.float32) * width * factor_of
    return jnp.minimum(jnp.maximum(array, -reach), reach).astype(kind)


def setup_inputs(seed: int = 0) -> dict:
    key_list = jax.random.split(jax.random.key(seed), 7)
    tokens = gaussian(key_list[0], (TOKENS, D), 1.0, 6.0, ((0, 4), (1, 4)))
    route_ids_keys = jax.random.split(jax.random.fold_in(key_list[1], 1), TOKENS // TOK)
    route_ids_turns = jax.random.permutation(jax.random.fold_in(key_list[1], 3), TOKENS // TOK)
    route_ids = jax.vmap(lambda own, number: routed_block(jax.random.fold_in(key_list[1], 2), own, number, TOK, EXPERTS, TOP, CAP, 2))(route_ids_keys, route_ids_turns).reshape((TOKENS, TOP))
    route_weights = jnp.clip(0.25 + 0.75 * jax.random.uniform(key_list[2], (TOKENS, TOP), jnp.float32) ** steps_of(key_list[2], (TOKENS, TOP), ((0, 4),), -0.2, 0.2), 0.25, 1.0)
    gate_weight = gaussian(key_list[3], (EXPERTS, D, FF), D ** -0.5, 0.09375, ((0, 4), (2, 8)))
    up_weight = gaussian(key_list[4], (EXPERTS, D, FF), D ** -0.5, 0.09375, ((0, 4), (2, 8)))
    down_weight = gaussian(key_list[5], (EXPERTS, FF, D), FF ** -0.5, 0.0625, ((0, 4), (1, 4), (2, 2)))
    return dict(tokens=tokens, route_ids=route_ids, route_weights=route_weights, gate_weight=gate_weight, up_weight=up_weight, down_weight=down_weight)


def run_expert(operands):
    expert_in, gate_block, up_block, down_block = operands
    gate = jnp.dot(expert_in, gate_block, preferred_element_type=jnp.float32)
    up = jnp.dot(expert_in, up_block, preferred_element_type=jnp.float32)
    hidden = (jax.nn.silu(gate) * up).astype(jnp.bfloat16)
    return jnp.dot(hidden, down_block, preferred_element_type=jnp.float32).astype(jnp.bfloat16)


def reference(tokens, route_ids, route_weights, gate_weight, up_weight, down_weight):
    pairs = TOKENS * TOP
    flat_ids = route_ids.reshape(-1).astype(jnp.int32)
    blocks = flat_ids.reshape(EXPERTS, TOK * TOP)
    onehot = (blocks[:, :, None] == jnp.arange(EXPERTS, dtype=jnp.int32)[None, None, :]).astype(jnp.int32)
    earlier = jnp.cumsum(onehot, axis=1) - onehot
    slot_index = jnp.sum(earlier * onehot, axis=2).reshape(-1).astype(jnp.int32)
    position = jnp.arange(pairs, dtype=jnp.int32)
    source = (position // (TOK * TOP)).astype(jnp.int32)
    row_index = (source * CAP + slot_index).astype(jnp.int32)
    token_index = (position // TOP).astype(jnp.int32)
    expert_in = jnp.zeros((EXPERTS, EXPERTS * CAP, D), tokens.dtype).at[flat_ids, row_index].set(tokens[token_index])
    expert_out = lax.map(run_expert, (expert_in, gate_weight, up_weight, down_weight))
    picked = expert_out[flat_ids, row_index].astype(jnp.float32).reshape(TOKENS, TOP, D)
    return jnp.sum(picked * route_weights[:, :, None], axis=1).astype(jnp.bfloat16)
```

```python
import functools

import jax
import jax.numpy as jnp
from jax import lax
from jax.experimental import pallas as pl
from jax.experimental.pallas import tpu as pltpu
from jax.sharding import PartitionSpec as P

MESH = pl.DeviceIdType.MESH


def plain(tokens, route_ids, route_weights, gate_weight, up_weight, down_weight):
    experts = lax.axis_size("expert")
    tok_rows, top_count = route_ids.shape
    capacity = 3 * tok_rows * top_count // (2 * experts)
    rows_total = experts * capacity
    flat_ids = route_ids.reshape(-1)
    onehot = (flat_ids[:, None] == jnp.arange(experts, dtype=jnp.int32)[None, :]).astype(jnp.int32)
    earlier = jnp.cumsum(onehot, axis=0) - onehot
    slot_index = jnp.sum(earlier * onehot, axis=1)
    destination = flat_ids * capacity + slot_index
    matches = (jnp.arange(rows_total, dtype=jnp.int32)[:, None] == destination[None, :]).astype(
        jnp.bfloat16
    )
    dispatch = jnp.sum(matches.reshape(rows_total, tok_rows, top_count), axis=2)
    outgoing = jnp.dot(dispatch, tokens, preferred_element_type=jnp.float32).astype(jnp.bfloat16)
    received = lax.all_to_all(
        outgoing.reshape(experts, capacity, tokens.shape[1]),
        "expert",
        split_axis=0,
        concat_axis=0,
        tiled=True,
    )
    received = received.reshape(rows_total, tokens.shape[1])
    piece = lax.all_gather(received, "section", axis=1, tiled=True)
    gate = jnp.dot(piece, gate_weight[0], preferred_element_type=jnp.float32)
    up = jnp.dot(piece, up_weight[0], preferred_element_type=jnp.float32)
    hidden = (jax.nn.silu(gate) * up).astype(jnp.bfloat16)
    partial_value = jnp.dot(
        lax.all_gather(hidden, "seq", axis=1, tiled=True),
        down_weight[0],
        preferred_element_type=jnp.float32,
    )
    summed = lax.psum_scatter(partial_value, "section", scatter_dimension=1, tiled=True)
    expert_out = summed.astype(jnp.bfloat16).reshape(experts, capacity, summed.shape[1])
    returned = lax.all_to_all(
        expert_out, "expert", split_axis=0, concat_axis=0, tiled=True
    ).reshape(rows_total, summed.shape[1])
    picked = (
        jnp.take(returned, destination, axis=0)
        .astype(jnp.float32)
        .reshape(tok_rows, top_count, summed.shape[1])
    )
    mixed = jnp.sum(picked * route_weights[:, :, None], axis=1).astype(jnp.bfloat16)
    return lax.all_gather(mixed, "section", axis=1, tiled=True)


def kernel(
    S, E, top, cap,
    tok_hbm, ids_hbm, weights_hbm, gate_hbm, up_hbm, down_hbm, out_hbm,
    T, IDS, RW, R, WG, WU, WD, DISP, WR, X, G, U, HO, HX, PO, CS, CR, ACC,
    YS, YR, PF, ZS, ZR, ZX, ZO, OUT,
    lsem, tsem, ssem, rsem, rrsem, hsem, csem, ysem, zsem, xsem, osem, dsem,
):
    s = lax.axis_index("section")
    e = lax.axis_index("expert")
    q = lax.axis_index("seq")
    core = e + 1 - 2 * lax.rem(e, 2)
    oy = lax.rem(e + 2, E)
    oyc = lax.rem(core + 2, E)
    oq = 1 - q
    rows = tok_hbm.shape[0]
    half = rows // 2
    feat = tok_hbm.shape[1]
    units = gate_hbm.shape[2]
    outs = down_hbm.shape[2]
    counter = [0]
    pending = []

    own = pltpu.make_async_copy(tok_hbm, T.at[s, pl.ds(pl.multiple_of(e * rows, rows), rows)], tsem.at[0])
    own.start()
    ids = pltpu.make_async_copy(ids_hbm, IDS, tsem.at[1])
    ids.start()
    route_weights = pltpu.make_async_copy(weights_hbm, RW, tsem.at[2])
    route_weights.start()

    barrier = pltpu.get_barrier_semaphore()
    partners = [{"section": lax.rem(s + j, S)} for j in range(1, S)]
    partners += [{"expert": core}, {"expert": oy}, {"expert": oyc}, {"seq": oq}]
    for p in partners:
        pl.semaphore_signal(barrier, inc=1, device_id=p, device_id_type=MESH)

    order = [0, 1, S - 1] + list(range(2, S - 1))
    loads = {}
    for i, j in enumerate(order):
        k = lax.rem(s + j, S)
        band = pl.ds(pl.multiple_of(k * feat, feat), feat)
        loads[j] = (
            pltpu.make_async_copy(gate_hbm.at[0, band], WG.at[band], lsem.at[2 * i]),
            pltpu.make_async_copy(up_hbm.at[0, band], WU.at[band], lsem.at[2 * i + 1]),
        )
    down_load = pltpu.make_async_copy(down_hbm.at[0], WD, lsem.at[2 * S])

    own.wait()
    ids.wait()
    route_weights.wait()
    R[e] = jnp.zeros(R.shape[1:], jnp.float32)
    R[e, 0:top, :] = IDS[...].astype(jnp.float32)
    R[e, top : 2 * top, :] = RW[...]
    pl.semaphore_wait(barrier, len(partners))

    def send(src, dst, recv, target, when=None):
        c = pltpu.make_async_remote_copy(
            src_ref=src, dst_ref=dst, send_sem=ssem.at[counter[0]], recv_sem=recv,
            device_id=target, device_id_type=MESH,
        )
        counter[0] += 1
        pending.append((when, c))
        if when is None:
            c.start()
        else:
            pl.when(when)(c.start)

    def arrived(ref, sem):
        pltpu.make_async_remote_copy(
            src_ref=ref, dst_ref=ref, send_sem=ssem.at[0], recv_sem=sem,
            device_id={"seq": oq}, device_id_type=MESH,
        ).wait_recv()

    def chunk(group, part, k):
        return T.at[k, pl.ds(pl.multiple_of(group * rows + part * half, half), half)]

    def slot(group, part, k):
        return rsem.at[(group * 2 + part) * S + k]

    def push(group, part, k, *targets):
        for t in targets:
            send(chunk(group, part, k), chunk(group, part, k), slot(group, part, k), t)

    def take(group, part, k):
        arrived(chunk(group, part, k), slot(group, part, k))

    to_x, to_y, to_core = {"seq": oq}, {"expert": oy}, {"expert": core}
    sec = [lax.rem(s + j, S) for j in range(S)]
    for j in order[1:]:
        push(e, q, s, {"section": sec[j]})
    for t, target in enumerate((core, oy, oyc)):
        send(R.at[e], R.at[e], rrsem.at[e], {"expert": target})
    push(e, q, s, to_y, to_core)
    push(e, oq, s, to_y, to_core)
    for j in order:
        for c in loads[j]:
            c.start()
    down_load.start()

    def from_z(j):
        take(e, q, sec[j])
        push(e, q, sec[j], to_x, to_y, to_core)

    def from_x(j, on):
        take(e, oq, sec[j])
        push(e, oq, sec[j], to_core, *([to_y] if on else []))

    def from_y(j, on):
        take(oy, q, sec[j])
        push(oy, q, sec[j], *([to_x] if on else []), to_core)

    def from_diag(j):
        take(oy, oq, sec[j])
        push(oy, oq, sec[j], to_core)

    def from_core(j):
        for group in (core, oyc):
            for part in (0, 1):
                take(group, part, sec[j])

    tile = min(256, units)

    def section_matmul(j, first, spans=None, then=None):
        from_core(j)
        for c in loads[j]:
            c.wait()
        k = sec[j]
        for g in range(E):
            X[g * cap : (g + 1) * cap, :] = jnp.dot(
                DISP[g], T[k, g * rows : (g + 1) * rows, :], preferred_element_type=jnp.float32
            ).astype(jnp.bfloat16)
        band = pl.ds(pl.multiple_of(k * feat, feat), feat)

        for n_span, r in enumerate(spans or [slice(None)]):

            @pl.loop(0, units // tile)
            def _(n):
                cols = pl.ds(pl.multiple_of(n * tile, tile), tile)
                for W, A in ((WG, G), (WU, U)):
                    v = jnp.dot(X[r, :], W[band, cols], preferred_element_type=jnp.float32)
                    if first:
                        A[r, cols] = v
                    else:
                        A[r, cols] = A[r, cols] + v

            if then is not None:
                then(n_span)

    for g in (core, oy, oyc):
        arrived(R.at[g], rrsem.at[g])
    me = e.astype(jnp.float32)
    before = (
        lax.broadcasted_iota(jnp.int32, (rows, rows), 0) < lax.broadcasted_iota(jnp.int32, (rows, rows), 1)
    ).astype(jnp.float32).astype(jnp.bfloat16)
    for g in range(E):
        table = R[g]
        named = jnp.zeros((1, rows), jnp.float32)
        weight = jnp.zeros((1, rows), jnp.float32)
        for n in range(top):
            hit = (table[n : n + 1, :] == me).astype(jnp.float32)
            named = named + hit
            weight = weight + hit * table[top + n : top + n + 1, :]
        rank = jnp.dot(
            jnp.broadcast_to(named, (8, rows)).astype(jnp.bfloat16), before, preferred_element_type=jnp.float32
        )[0:1, :]
        place = lax.broadcasted_iota(jnp.int32, (cap, rows), 0).astype(jnp.float32)
        match = jnp.where(place == rank, 1.0, 0.0) * named
        DISP[g] = match.astype(jnp.bfloat16)
        WR[g] = jnp.broadcast_to(jnp.sum(match * weight, axis=1, keepdims=True), (cap, WR.shape[2]))

    from_z(order[1])
    take(oy, q, s)
    take(oy, oq, s)
    push(oy, q, s, to_core)
    push(oy, oq, s, to_core)
    others = order[1:]
    onward = {j: i < (S - 2) // 2 for i, j in enumerate(others)}
    for i, j in enumerate(others):
        if i + 1 < len(others):
            from_z(others[i + 1])
        from_x(j, onward[j])
        from_y(j, not onward[j])
        if i > 0:
            from_diag(others[i - 1])
        if i == len(others) - 2:
            section_matmul(0, True)
    for j in others[:-1]:
        section_matmul(j, False)
    from_diag(others[-1])
    near = e - lax.rem(e, 2)
    far = lax.rem(near + 2, E)
    groups = [far, far + 1, near, near + 1]

    def span(g):
        return pl.ds(pl.multiple_of(g * cap, cap), cap)

    def hidden_out(n_span):
        for i in (2 * n_span, 2 * n_span + 1):
            g = groups[i]
            a = G[span(g), 0:units]
            HO[span(g), :] = (a / (1.0 + jnp.exp(-a)) * U[span(g), :]).astype(jnp.bfloat16)
            send(HO.at[span(g)], HX.at[span(g)], hsem.at[i], to_x)

    def chip_span(y):
        return pl.ds(pl.multiple_of(y * 2 * cap, 2 * cap), 2 * cap)

    section_matmul(others[-1], False, [chip_span(oy // 2), chip_span(e // 2)], hidden_out)

    down_load.wait()
    own_units = pl.ds(pl.multiple_of(q * units, units), units)
    other_units = pl.ds(pl.multiple_of(oq * units, units), units)
    otile = min(256, outs)

    @pl.loop(0, outs // otile)
    def _(n):
        cols = pl.ds(pl.multiple_of(n * otile, otile), otile)
        PO[:, cols] = jnp.dot(HO[...], WD[own_units, cols], preferred_element_type=jnp.float32)

    side = lax.rem(e, 2)
    part = outs // 2
    chunks = YS.shape[1]
    width = part // chunks
    mine, theirs = side * part, (1 - side) * part
    inner = (s == 1) | (s == 2)
    outer = (s == 0) | (s == 3)
    in_sec = jnp.where(s == 0, 1, 2)
    cross = 3 - s
    out_sec = jnp.where(s == 1, 0, 3)

    def half(g, base, put):
        @pl.loop(0, part // otile)
        def _(n):
            cols = pl.ds(pl.multiple_of(base + n * otile, otile), otile)
            v = PO[span(g), cols] + jnp.dot(
                HX[span(g), :], WD[other_units, cols], preferred_element_type=jnp.float32
            )
            v = (v * WR[g][:, 0:1]).astype(jnp.bfloat16)
            v = lax.dot_general(DISP[g], v, (((0,), (0,)), ((), ())), preferred_element_type=jnp.float32)
            put(pl.ds(pl.multiple_of(n * otile, otile), otile), v)

    def to_partner(i):
        def put(cols, v):
            CS[i, :, cols] = v.astype(jnp.bfloat16)

        half(groups[i], theirs, put)
        send(CS.at[i], CR.at[i], csem.at[i], to_core)

    def keep(i):
        def put(cols, v):
            ACC[i, :, cols] = v

        half(groups[i], mine, put)
        arrived(CR.at[i], csem.at[i])

    def piece(i, n):
        cols = slice(n * width, (n + 1) * width)
        return ACC[i, :, cols] + CR[i, :, cols].astype(jnp.float32)

    def to_neighbour(i):
        for n in range(chunks):
            YS[i, n] = piece(i, n).astype(jnp.bfloat16)
            send(YS.at[i, n], YR.at[i, n], ysem.at[i, n], to_y)

    def first(a, n):
        arrived(YR.at[a, n], ysem.at[a, n])
        total = piece(2 + a, n) + YR[a, n].astype(jnp.float32)

        @pl.when(outer)
        def _():
            ZS[a, n] = total.astype(jnp.bfloat16)

        @pl.when(inner)
        def _():
            PF[a, n] = total

        send(ZS.at[a, n], ZR.at[a, n], zsem.at[a, n], {"section": in_sec}, outer)

    def second(a, n):
        @pl.when(inner)
        def _():
            arrived(ZR.at[a, n], zsem.at[a, n])
            ZS[a, n] = (PF[a, n] + ZR[a, n].astype(jnp.float32)).astype(jnp.bfloat16)

        send(ZS.at[a, n], ZX.at[a, n], xsem.at[a, n], {"section": cross}, inner)

    drains = []

    def drain(h, n, k):
        cols = pl.ds(pl.multiple_of(h * part + n * width, width), width)
        c = pltpu.make_async_copy(OUT.at[h, n], out_hbm.at[:, cols], dsem.at[k, n])
        c.start()
        drains.append(c)

    def third(a, n):
        @pl.when(inner)
        def _():
            arrived(ZX.at[a, n], xsem.at[a, n])
            total = (ZS[a, n].astype(jnp.float32) + ZX[a, n].astype(jnp.float32)).astype(jnp.bfloat16)
            ZO[a, n] = total

            @pl.when(side == a)
            def _():
                OUT[side, n] = total

        send(ZO.at[a, n], OUT.at[side, n], osem.at[side, n], {"section": out_sec, "expert": near + a}, inner)
        send(ZO.at[a, n], OUT.at[side, n], osem.at[side, n], to_core, inner & (side != a))

    def hidden_in(i):
        arrived(HX.at[span(groups[i])], hsem.at[i])

    for i in (0, 1):
        hidden_in(i)
        to_partner(i)
        keep(i)
        to_neighbour(i)
    hidden_in(2)
    to_partner(2)
    keep(2)
    steps = [functools.partial(second, 0, n) for n in range(chunks)]
    for n in range(chunks):
        first(0, n)
    cut = chunks // 4
    for f in steps[:cut]:
        f()
    hidden_in(3)
    to_partner(3)
    for f in steps[cut : 2 * cut]:
        f()
    keep(3)
    for n in range(chunks):
        first(1, n)
    steps = steps[2 * cut :] + [functools.partial(third, 0, n) for n in range(chunks)]
    lag = chunks // 2
    for n in range(chunks + lag):
        if n < chunks:
            for f in steps[n * len(steps) // chunks : (n + 1) * len(steps) // chunks]:
                f()
            second(1, n)
        if n >= lag:
            third(1, n - lag)

    for n in range(chunks):

        @pl.when(outer)
        def _():
            arrived(OUT.at[side, n], osem.at[side, n])

        drain(side, n, 0)
    for n in range(chunks):
        arrived(OUT.at[1 - side, n], osem.at[1 - side, n])
        drain(1 - side, n, 1)
    for c in drains:
        c.wait()
    for when, c in pending:
        if when is None:
            c.wait_send()
        else:
            pl.when(when)(c.wait_send)


def fused(tokens, route_ids, route_weights, gate_weight, up_weight, down_weight):
    S, E = lax.axis_size("section"), lax.axis_size("expert")
    rows, feat = tokens.shape
    top = route_ids.shape[1]
    cap = 3 * rows * top // (2 * E)
    units, outs = gate_weight.shape[2], down_weight.shape[2]
    table_rows = -(-2 * top // 8) * 8
    bf, f32 = jnp.bfloat16, jnp.float32
    dma = pltpu.SemaphoreType.DMA
    sends = 256
    part, chunks = outs // 2, outs // 256
    grid = (2, chunks, rows, part // chunks)
    return pl.pallas_call(
        functools.partial(kernel, S, E, top, cap),
        out_shape=jax.ShapeDtypeStruct((rows, outs), bf),
        in_specs=[pl.BlockSpec(memory_space=pl.ANY)] * 6,
        out_specs=pl.BlockSpec(memory_space=pl.ANY),
        scratch_shapes=[
            pltpu.VMEM((S, E * rows, feat), bf),
            pltpu.VMEM((top, rows), jnp.int32),
            pltpu.VMEM((top, rows), f32),
            pltpu.VMEM((E, table_rows, rows), f32),
            pltpu.VMEM((S * feat, units), bf),
            pltpu.VMEM((S * feat, units), bf),
            pltpu.VMEM(down_weight.shape[1:], bf),
            pltpu.VMEM((E, cap, rows), bf),
            pltpu.VMEM((E, cap, 128), f32),
            pltpu.VMEM((E * cap, feat), bf),
            pltpu.VMEM((E * cap, units), f32),
            pltpu.VMEM((E * cap, units), f32),
            pltpu.VMEM((E * cap, units), bf),
            pltpu.VMEM((E * cap, units), bf),
            pltpu.VMEM((E * cap, outs), f32),
            pltpu.VMEM((4, rows, part), bf),
            pltpu.VMEM((4, rows, part), bf),
            pltpu.VMEM((4, rows, part), f32),
            pltpu.VMEM(grid, bf),
            pltpu.VMEM(grid, bf),
            pltpu.VMEM(grid, f32),
            pltpu.VMEM(grid, bf),
            pltpu.VMEM(grid, bf),
            pltpu.VMEM(grid, bf),
            pltpu.VMEM(grid, bf),
            pltpu.VMEM(grid, bf),
            dma((2 * S + 1,)),
            dma((3,)),
            dma((sends,)),
            dma((2 * E * S,)),
            dma((E,)),
            dma((4,)),
            dma((4,)),
            dma((2, chunks)),
            dma((2, chunks)),
            dma((2, chunks)),
            dma((2, chunks)),
            dma((2, chunks)),
        ],
        compiler_params=pltpu.CompilerParams(
            collective_id=0, has_side_effects=True, vmem_limit_bytes=60 * 1024 * 1024
        ),
    )(tokens, route_ids.T, route_weights.T, gate_weight, up_weight, down_weight)


def shards(tokens, route_ids, route_weights, gate_weight, up_weight, down_weight):
    args = (tokens, route_ids, route_weights, gate_weight, up_weight, down_weight)
    pairs = lax.axis_size("expert") == 2 * 2 and lax.axis_size("seq") == 2
    if pairs and lax.axis_size("section") == 4:
        return fused(*args)
    return plain(*args)


def solution(mesh):
    in_specs = (
        P("expert", "section"),
        P("expert", None),
        P("expert", None),
        P("expert", None, ("section", "seq")),
        P("expert", None, ("section", "seq")),
        P("expert", "section", "seq"),
    )
    out_specs = P("expert", "seq")
    return jax.shard_map(shards, mesh=mesh, in_specs=in_specs, out_specs=out_specs, check_vma=False)
```

```python
import functools

import jax
import jax.numpy as jnp
from jax import lax
from jax.experimental import pallas as pl
from jax.experimental.pallas import tpu as pltpu
from jax.sharding import PartitionSpec as P

MESH = pl.DeviceIdType.MESH


def plain(tokens, route_ids, route_weights, gate_weight, up_weight, down_weight):
    experts = lax.axis_size("expert")
    tok_rows, top_count = route_ids.shape
    capacity = 3 * tok_rows * top_count // (2 * experts)
    rows_total = experts * capacity
    flat_ids = route_ids.reshape(-1)
    onehot = (flat_ids[:, None] == jnp.arange(experts, dtype=jnp.int32)[None, :]).astype(jnp.int32)
    earlier = jnp.cumsum(onehot, axis=0) - onehot
    slot_index = jnp.sum(earlier * onehot, axis=1)
    destination = flat_ids * capacity + slot_index
    matches = (jnp.arange(rows_total, dtype=jnp.int32)[:, None] == destination[None, :]).astype(
        jnp.bfloat16
    )
    dispatch = jnp.sum(matches.reshape(rows_total, tok_rows, top_count), axis=2)
    outgoing = jnp.dot(dispatch, tokens, preferred_element_type=jnp.float32).astype(jnp.bfloat16)
    received = lax.all_to_all(
        outgoing.reshape(experts, capacity, tokens.shape[1]),
        "expert",
        split_axis=0,
        concat_axis=0,
        tiled=True,
    )
    received = received.reshape(rows_total, tokens.shape[1])
    piece = lax.all_gather(received, "section", axis=1, tiled=True)
    gate = jnp.dot(piece, gate_weight[0], preferred_element_type=jnp.float32)
    up = jnp.dot(piece, up_weight[0], preferred_element_type=jnp.float32)
    hidden = (jax.nn.silu(gate) * up).astype(jnp.bfloat16)
    partial_value = jnp.dot(
        lax.all_gather(hidden, "seq", axis=1, tiled=True),
        down_weight[0],
        preferred_element_type=jnp.float32,
    )
    summed = lax.psum_scatter(partial_value, "section", scatter_dimension=1, tiled=True)
    expert_out = summed.astype(jnp.bfloat16).reshape(experts, capacity, summed.shape[1])
    returned = lax.all_to_all(
        expert_out, "expert", split_axis=0, concat_axis=0, tiled=True
    ).reshape(rows_total, summed.shape[1])
    picked = (
        jnp.take(returned, destination, axis=0)
        .astype(jnp.float32)
        .reshape(tok_rows, top_count, summed.shape[1])
    )
    mixed = jnp.sum(picked * route_weights[:, :, None], axis=1).astype(jnp.bfloat16)
    return lax.all_gather(mixed, "section", axis=1, tiled=True)


def kernel(
    S, E, top, cap,
    tok_hbm, ids_hbm, weights_hbm, gate_hbm, up_hbm, down_hbm, out_hbm,
    T, IDS, RW, R, WG, WU, WD, DISP, WR, G, U, HO, HX, PO, CS, CR, ACC,
    YS, YR, PF, ZS, ZR, ZX, ZO, OUT,
    lsem, tsem, ssem, rsem, rrsem, hsem, csem, ysem, zsem, xsem, osem, dsem,
):
    s = lax.axis_index("section")
    e = lax.axis_index("expert")
    q = lax.axis_index("seq")
    side = lax.rem(e, 2)
    core = e + 1 - 2 * side
    near = e - side
    far = lax.rem(near + 2, E)
    oy = lax.rem(e + 2, E)
    oyc = lax.rem(core + 2, E)
    oq = 1 - q
    rows = tok_hbm.shape[0]
    block_rows = rows // 2
    feat = tok_hbm.shape[1]
    units = gate_hbm.shape[2]
    outs = down_hbm.shape[2]
    inner = (s == 1) | (s == 2)
    outer = (s == 0) | (s == 3)
    in_sec = jnp.where(s == 0, 1, 2)
    cross = 3 - s
    out_sec = jnp.where(s == 1, 0, 3)

    own = pltpu.make_async_copy(tok_hbm, T.at[s, pl.ds(pl.multiple_of(e * rows, rows), rows)], tsem.at[0])
    own.start()
    ids = pltpu.make_async_copy(ids_hbm, IDS, tsem.at[1])
    ids.start()
    route_weights = pltpu.make_async_copy(weights_hbm, RW, tsem.at[2])
    route_weights.start()

    to_x, to_y, to_core = {"seq": oq}, {"expert": oy}, {"expert": core}
    up, down, skip = ({"section": lax.rem(s + j, S)} for j in (1, S - 1, 2))
    barrier = pltpu.get_barrier_semaphore()
    for p, when in (
        (to_core, None), (to_x, None), (to_y, None), ({"expert": oyc}, None),
        (skip, None), (up, s != S - 1), (down, s != 0),
    ):
        def signal(p=p):
            pl.semaphore_signal(barrier, inc=1, device_id=p, device_id_type=MESH)

        if when is None:
            signal()
        else:
            pl.when(when)(signal)

    step = 1 + 2 * lax.rem(s, 2)
    sec = [s, lax.rem(s + 2, S), lax.rem(s + step, S), lax.rem(s + S - step, S)]
    bands = [pl.ds(pl.multiple_of(k * feat, feat), feat) for k in sec]
    loads = [
        (
            pltpu.make_async_copy(gate_hbm.at[0, band], WG.at[band], lsem.at[2 * i]),
            pltpu.make_async_copy(up_hbm.at[0, band], WU.at[band], lsem.at[2 * i + 1]),
        )
        for i, band in enumerate(bands)
    ]
    down_load = pltpu.make_async_copy(down_hbm.at[0], WD, lsem.at[2 * S])

    own.wait()
    for pair in loads:
        for c in pair:
            c.start()
    down_load.start()
    ids.wait()
    route_weights.wait()
    R[e] = jnp.zeros(R.shape[1:], jnp.float32)
    R[e, 0:top, :] = IDS[...].astype(jnp.float32)
    R[e, top : 2 * top, :] = RW[...]
    pl.semaphore_wait(barrier, 6 + inner.astype(jnp.int32))

    def send(kind, src, dst, recv, target, when=None):
        c = pltpu.make_async_remote_copy(
            src_ref=src, dst_ref=dst, send_sem=ssem.at[kind], recv_sem=recv,
            device_id=target, device_id_type=MESH,
        )
        if when is None:
            c.start()
        else:
            pl.when(when)(c.start)

    def arrived(ref, sem):
        pltpu.make_async_remote_copy(
            src_ref=ref, dst_ref=ref, send_sem=ssem.at[0], recv_sem=sem,
            device_id={"seq": oq}, device_id_type=MESH,
        ).wait_recv()

    def sent(kind, ref):
        pltpu.make_async_remote_copy(
            src_ref=ref, dst_ref=ref, send_sem=ssem.at[kind], recv_sem=ssem.at[kind],
            device_id={"seq": oq}, device_id_type=MESH,
        ).wait_send()

    def chunk(group, part, k):
        return T.at[k, pl.ds(pl.multiple_of(group * rows + part * block_rows, block_rows), block_rows)]

    def slot(group, part, k):
        return rsem.at[(group * 2 + part) * S + k]

    def push(kind, group, part, k, target, when=None):
        send(kind, chunk(group, part, k), chunk(group, part, k), slot(group, part, k), target, when)

    def take(group, part, k):
        arrived(chunk(group, part, k), slot(group, part, k))

    for target in (to_core, {"expert": oyc}, to_y):
        send(3, R.at[e], R.at[e], rrsem.at[e], target)
    push(0, e, 1 - side, s, to_core)
    push(0, e, side, s, to_core)

    def nearest(n):
        push(2, near + n, side, s, up, s != S - 1)
        push(2, near + n, side, s, down, s != 0)

    for n in (0, 1):

        @pl.when(side != n)
        def _():
            take(near + n, side, s)

        push(2, near + n, side, s, skip)
        if n == 0:
            nearest(n)
        push(1, near + n, side, s, to_y)

    me = e.astype(jnp.float32)
    before = (
        lax.broadcasted_iota(jnp.int32, (rows, rows), 0) < lax.broadcasted_iota(jnp.int32, (rows, rows), 1)
    ).astype(jnp.float32).astype(jnp.bfloat16)

    def dispatch(g):
        table = R[g]
        named = jnp.zeros((1, rows), jnp.float32)
        weight = jnp.zeros((1, rows), jnp.float32)
        for n in range(top):
            hit = (table[n : n + 1, :] == me).astype(jnp.float32)
            named = named + hit
            weight = weight + hit * table[top + n : top + n + 1, :]
        rank = jnp.dot(
            jnp.broadcast_to(named, (8, rows)).astype(jnp.bfloat16), before, preferred_element_type=jnp.float32
        )[0:1, :]
        place = lax.broadcasted_iota(jnp.int32, (cap, rows), 0).astype(jnp.float32)
        match = jnp.where(place == rank, 1.0, 0.0) * named
        DISP[g] = match.astype(jnp.bfloat16)
        WR[g] = jnp.broadcast_to(jnp.sum(match * weight, axis=1, keepdims=True), (cap, WR.shape[2]))

    def z_in(n, i, when=None):
        if when is not None:
            pl.when(when)(functools.partial(z_in, n, i))
            return
        take(near + n, side, sec[i])
        if i == 1:
            push(2, near + n, side, sec[i], {"section": out_sec}, inner)
        push(1, near + n, side, sec[i], to_y)
        push(0, near + n, side, sec[i], to_core)

    def y_in(n, i):
        take(far + n, side, sec[i])
        push(0, far + n, side, sec[i], to_core)

    groups = [near, far, near + 1, far + 1]
    loaded = set()

    def span(g):
        return pl.ds(pl.multiple_of(g * cap, cap), cap)

    def block(m, i):
        g, k = groups[m], sec[i]
        if m % 2 == 0 and i == 0:

            @pl.when(side != m // 2)
            def _():
                take(g, 1 - side, k)
        else:
            take(g, 1 - side, k)
        if i not in loaded:
            loaded.add(i)
            for c in loads[i]:
                c.wait()
        lines = pl.ds(pl.multiple_of(g * rows, rows), rows)
        for W, A in ((WG, G), (WU, U)):
            v = jnp.dot(T[k, lines, :], W[bands[i], :], preferred_element_type=jnp.float32)
            if i == 0:
                A[m] = v
            else:
                A[m] = A[m] + v

    def hidden_out(m):
        a = G[m]
        h = (a / (1.0 + jnp.exp(-a)) * U[m]).astype(jnp.bfloat16)
        HO[m] = jnp.dot(DISP[groups[m]], h, preferred_element_type=jnp.float32).astype(jnp.bfloat16)
        send(4, HO.at[m], HX.at[m], hsem.at[m], to_x)

    own_units = pl.ds(pl.multiple_of(q * units, units), units)
    other_units = pl.ds(pl.multiple_of(oq * units, units), units)
    part = outs // 2
    chunks = YS.shape[1]
    width = part // chunks
    mine, theirs = (pl.ds(pl.multiple_of(h * part, part), part) for h in (side, 1 - side))

    def ahead(m):
        if m == 1:
            down_load.wait()
        PO[m] = jnp.dot(HO[m], WD[own_units, :], preferred_element_type=jnp.float32)

    def half(m, cols):
        g = groups[m]
        v = PO[m, :, cols] + jnp.dot(HX[m], WD[other_units, cols], preferred_element_type=jnp.float32)
        v = (v * WR[g][:, 0:1]).astype(jnp.bfloat16)
        return lax.dot_general(DISP[g], v, (((0,), (0,)), ((), ())), preferred_element_type=jnp.float32)

    def to_partner(m):
        CS[m] = half(m, theirs).astype(jnp.bfloat16)
        send(5, CS.at[m], CR.at[m], csem.at[m], to_core)

    def keep(m):
        ACC[m] = half(m, mine)
        arrived(CR.at[m], csem.at[m])

    def piece(m, n):
        cols = slice(n * width, (n + 1) * width)
        return ACC[m, :, cols] + CR[m, :, cols].astype(jnp.float32)

    def to_neighbour(b):
        for n in range(chunks):
            YS[b, n] = piece(2 * b + 1, n).astype(jnp.bfloat16)
            send(6, YS.at[b, n], YR.at[b, n], ysem.at[b, n], to_y)

    def first(a, n):
        arrived(YR.at[a, n], ysem.at[a, n])
        total = piece(2 * a, n) + YR[a, n].astype(jnp.float32)

        @pl.when(outer)
        def _():
            ZS[a, n] = total.astype(jnp.bfloat16)

        @pl.when(inner)
        def _():
            PF[a, n] = total

        send(7, ZS.at[a, n], ZR.at[a, n], zsem.at[a, n], {"section": in_sec}, outer)

    def second(a, n):
        @pl.when(inner)
        def _():
            arrived(ZR.at[a, n], zsem.at[a, n])
            ZS[a, n] = (PF[a, n] + ZR[a, n].astype(jnp.float32)).astype(jnp.bfloat16)

        send(7, ZS.at[a, n], ZX.at[a, n], xsem.at[a, n], {"section": cross}, inner)

    def drain(h):
        for n in range(chunks):
            cols = pl.ds(pl.multiple_of(h * part + n * width, width), width)
            out_hbm[:, cols] = OUT[h, n]

    def third(a, n):
        @pl.when(inner)
        def _():
            arrived(ZX.at[a, n], xsem.at[a, n])
            total = (ZS[a, n].astype(jnp.float32) + ZX[a, n].astype(jnp.float32)).astype(jnp.bfloat16)
            ZO[a, n] = total

            @pl.when(side == a)
            def _():
                OUT[side, n] = total

        send(8, ZO.at[a, n], OUT.at[side, n], osem.at[side], {"section": out_sec, "expert": near + a}, inner)
        send(9, ZO.at[a, n], OUT.at[side, n], osem.at[side], to_core, inner & (side != a))

    def hidden_in(m):
        arrived(HX.at[m], hsem.at[m])

    block(0, 0)
    for g in (core, oy, oyc):
        arrived(R.at[g], rrsem.at[g])
    block(2, 0)
    dispatch(near)
    dispatch(far)
    dispatch(near + 1)
    dispatch(far + 1)
    y_in(0, 0)
    z_in(0, 1)
    nearest(1)
    z_in(0, 2)
    block(1, 0)
    y_in(1, 0)
    block(0, 1)
    block(0, 2)
    z_in(0, 3)
    z_in(1, 1, inner)
    block(3, 0)
    y_in(0, 1)
    block(0, 3)
    hidden_out(0)
    block(1, 1)
    z_in(1, 1, outer)
    z_in(1, 2)
    y_in(0, 2)
    block(2, 1)
    z_in(1, 3, inner)
    y_in(0, 3)
    z_in(1, 3, outer)
    block(1, 2)
    block(2, 2)
    block(1, 3)
    hidden_out(1)
    y_in(1, 1)
    block(2, 3)
    hidden_out(2)
    ahead(1)
    block(3, 1)
    ahead(0)
    y_in(1, 2)
    hidden_in(0)
    to_partner(0)
    block(3, 2)
    y_in(1, 3)
    keep(0)
    block(3, 3)
    hidden_out(3)
    hidden_in(1)
    to_partner(1)
    keep(1)
    to_neighbour(0)
    ahead(2)
    ahead(3)
    hidden_in(2)
    to_partner(2)
    keep(2)
    cut = chunks // 2
    for n in range(cut):
        first(0, n)
    hidden_in(3)
    to_partner(3)
    for n in range(cut, cut + 2):
        first(0, n)
    keep(3)
    to_neighbour(1)
    for n in range(cut + 2, chunks):
        first(0, n)
    for n in range(chunks):
        second(0, n)
    for n in range(chunks + 2 * cut):
        if n < chunks:
            third(0, n)
            first(1, n)
        if cut <= n < chunks + cut:
            second(1, n - cut)
        if n >= 2 * cut:
            third(1, n - 2 * cut)

    @pl.when(outer)
    def _():
        arrived(OUT.at[side], osem.at[side])

    drain(side)
    arrived(OUT.at[1 - side], osem.at[1 - side])
    drain(1 - side)
    sent(0, T.at[0:2])
    sent(1, T.at[0])
    sent(3, R.at[0:3])
    sent(4, HO)
    sent(5, CS)
    sent(6, YS)
    sent(7, ZS)

    @pl.when(outer)
    def _():
        sent(2, T.at[0, 0 : 2 * rows])

    @pl.when(inner)
    def _():
        sent(2, T.at[0])
        sent(8, ZO)
        sent(9, ZO.at[0])


def fused(tokens, route_ids, route_weights, gate_weight, up_weight, down_weight):
    S, E = lax.axis_size("section"), lax.axis_size("expert")
    rows, feat = tokens.shape
    top = route_ids.shape[1]
    cap = 3 * rows * top // (2 * E)
    units, outs = gate_weight.shape[2], down_weight.shape[2]
    table_rows = -(-2 * top // 8) * 8
    bf, f32 = jnp.bfloat16, jnp.float32
    dma = pltpu.SemaphoreType.DMA
    sends = 10
    part, chunks = outs // 2, outs // 256
    grid = (2, chunks, rows, part // chunks)
    return pl.pallas_call(
        functools.partial(kernel, S, E, top, cap),
        out_shape=pltpu.VMEM((rows, outs), bf),
        in_specs=[pl.BlockSpec(memory_space=pl.ANY)] * 6,
        out_specs=pl.BlockSpec(memory_space=pltpu.VMEM),
        scratch_shapes=[
            pltpu.VMEM((S, E * rows, feat), bf),
            pltpu.VMEM((top, rows), jnp.int32),
            pltpu.VMEM((top, rows), f32),
            pltpu.VMEM((E, table_rows, rows), f32),
            pltpu.VMEM((S * feat, units), bf),
            pltpu.VMEM((S * feat, units), bf),
            pltpu.VMEM(down_weight.shape[1:], bf),
            pltpu.VMEM((E, cap, rows), bf),
            pltpu.VMEM((E, cap, 128), f32),
            pltpu.VMEM((E, rows, units), f32),
            pltpu.VMEM((E, rows, units), f32),
            pltpu.VMEM((E, cap, units), bf),
            pltpu.VMEM((E, cap, units), bf),
            pltpu.VMEM((E, cap, outs), f32),
            pltpu.VMEM((4, rows, part), bf),
            pltpu.VMEM((4, rows, part), bf),
            pltpu.VMEM((4, rows, part), f32),
            pltpu.VMEM(grid, bf),
            pltpu.VMEM(grid, bf),
            pltpu.VMEM(grid, f32),
            pltpu.VMEM(grid, bf),
            pltpu.VMEM(grid, bf),
            pltpu.VMEM(grid, bf),
            pltpu.VMEM(grid, bf),
            pltpu.VMEM(grid, bf),
            dma((2 * S + 1,)),
            dma((3,)),
            dma((sends,)),
            dma((2 * E * S,)),
            dma((E,)),
            dma((4,)),
            dma((4,)),
            dma((2, chunks)),
            dma((2, chunks)),
            dma((2, chunks)),
            dma((2,)),
            dma((1,)),
        ],
        compiler_params=pltpu.CompilerParams(
            collective_id=0, has_side_effects=True, vmem_limit_bytes=60 * 1024 * 1024
        ),
    )(tokens, route_ids.T, route_weights.T, gate_weight, up_weight, down_weight)


def shards(tokens, route_ids, route_weights, gate_weight, up_weight, down_weight):
    args = (tokens, route_ids, route_weights, gate_weight, up_weight, down_weight)
    pairs = lax.axis_size("expert") == 2 * 2 and lax.axis_size("seq") == 2
    if pairs and lax.axis_size("section") == 4:
        return fused(*args)
    return plain(*args)


def solution(mesh):
    in_specs = (
        P("expert", "section"),
        P("expert", None),
        P("expert", None),
        P("expert", None, ("section", "seq")),
        P("expert", None, ("section", "seq")),
        P("expert", "section", "seq"),
    )
    out_specs = P("expert", "seq")
    return jax.shard_map(shards, mesh=mesh, in_specs=in_specs, out_specs=out_specs, check_vma=False)
```

```python
import functools

import jax
import jax.numpy as jnp
from jax import lax
from jax.experimental import pallas as pl
from jax.experimental.pallas import tpu as pltpu
from jax.sharding import PartitionSpec as P

MESH = pl.DeviceIdType.MESH


def plain(tokens, route_ids, route_weights, gate_weight, up_weight, down_weight):
    experts = lax.axis_size("expert")
    tok_rows, top_count = route_ids.shape
    capacity = 3 * tok_rows * top_count // (2 * experts)
    rows_total = experts * capacity
    flat_ids = route_ids.reshape(-1)
    onehot = (flat_ids[:, None] == jnp.arange(experts, dtype=jnp.int32)[None, :]).astype(jnp.int32)
    earlier = jnp.cumsum(onehot, axis=0) - onehot
    slot_index = jnp.sum(earlier * onehot, axis=1)
    destination = flat_ids * capacity + slot_index
    matches = (jnp.arange(rows_total, dtype=jnp.int32)[:, None] == destination[None, :]).astype(
        jnp.bfloat16
    )
    dispatch = jnp.sum(matches.reshape(rows_total, tok_rows, top_count), axis=2)
    outgoing = jnp.dot(dispatch, tokens, preferred_element_type=jnp.float32).astype(jnp.bfloat16)
    received = lax.all_to_all(
        outgoing.reshape(experts, capacity, tokens.shape[1]),
        "expert",
        split_axis=0,
        concat_axis=0,
        tiled=True,
    )
    received = received.reshape(rows_total, tokens.shape[1])
    piece = lax.all_gather(received, "section", axis=1, tiled=True)
    gate = jnp.dot(piece, gate_weight[0], preferred_element_type=jnp.float32)
    up = jnp.dot(piece, up_weight[0], preferred_element_type=jnp.float32)
    hidden = (jax.nn.silu(gate) * up).astype(jnp.bfloat16)
    partial_value = jnp.dot(
        lax.all_gather(hidden, "seq", axis=1, tiled=True),
        down_weight[0],
        preferred_element_type=jnp.float32,
    )
    summed = lax.psum_scatter(partial_value, "section", scatter_dimension=1, tiled=True)
    expert_out = summed.astype(jnp.bfloat16).reshape(experts, capacity, summed.shape[1])
    returned = lax.all_to_all(
        expert_out, "expert", split_axis=0, concat_axis=0, tiled=True
    ).reshape(rows_total, summed.shape[1])
    picked = (
        jnp.take(returned, destination, axis=0)
        .astype(jnp.float32)
        .reshape(tok_rows, top_count, summed.shape[1])
    )
    mixed = jnp.sum(picked * route_weights[:, :, None], axis=1).astype(jnp.bfloat16)
    return lax.all_gather(mixed, "section", axis=1, tiled=True)


def kernel(
    S, E, top, cap,
    tok_hbm, ids_hbm, weights_hbm, gate_hbm, up_hbm, down_hbm, out_hbm,
    T, IDS, RW, R, WG, WU, WD, DISP, WR, G, U, HO, HX, PO, CS, CR, ACC,
    YS, YR, PF, ZS, ZR, ZX, ZO, OUT,
    lsem, tsem, ssem, rsem, rrsem, hsem, csem, ysem, zsem, xsem, osem, dsem,
):
    s = lax.axis_index("section")
    e = lax.axis_index("expert")
    q = lax.axis_index("seq")
    side = lax.rem(e, 2)
    core = e + 1 - 2 * side
    near = e - side
    far = lax.rem(near + 2, E)
    oy = lax.rem(e + 2, E)
    oyc = lax.rem(core + 2, E)
    oq = 1 - q
    rows = tok_hbm.shape[0]
    block_rows = rows // 2
    feat = tok_hbm.shape[1]
    units = gate_hbm.shape[2]
    outs = down_hbm.shape[2]
    inner = (s == 1) | (s == 2)
    outer = (s == 0) | (s == 3)
    in_sec = jnp.where(s == 0, 1, 2)
    cross = 3 - s
    out_sec = jnp.where(s == 1, 0, 3)

    own = pltpu.make_async_copy(tok_hbm, T.at[s, pl.ds(pl.multiple_of(e * rows, rows), rows)], tsem.at[0])
    own.start()
    ids = pltpu.make_async_copy(ids_hbm, IDS, tsem.at[1])
    ids.start()
    route_weights = pltpu.make_async_copy(weights_hbm, RW, tsem.at[2])
    route_weights.start()

    to_x, to_y, to_core = {"seq": oq}, {"expert": oy}, {"expert": core}
    up, down, skip = ({"section": lax.rem(s + j, S)} for j in (1, S - 1, 2))
    barrier = pltpu.get_barrier_semaphore()
    for p, when in (
        (to_core, None), (to_x, None), (to_y, None), ({"expert": oyc}, None),
        (skip, None), (up, s != S - 1), (down, s != 0),
    ):
        def signal(p=p):
            pl.semaphore_signal(barrier, inc=1, device_id=p, device_id_type=MESH)

        if when is None:
            signal()
        else:
            pl.when(when)(signal)

    step = 1 + 2 * lax.rem(s, 2)
    sec = [s, lax.rem(s + 2, S), lax.rem(s + step, S), lax.rem(s + S - step, S)]
    bands = [pl.ds(pl.multiple_of(k * feat, feat), feat) for k in sec]
    loads = [
        (
            pltpu.make_async_copy(gate_hbm.at[0, band], WG.at[band], lsem.at[2 * i]),
            pltpu.make_async_copy(up_hbm.at[0, band], WU.at[band], lsem.at[2 * i + 1]),
        )
        for i, band in enumerate(bands)
    ]
    down_load = pltpu.make_async_copy(down_hbm.at[0], WD, lsem.at[2 * S])

    own.wait()
    for pair in loads:
        for c in pair:
            c.start()
    down_load.start()
    ids.wait()
    route_weights.wait()
    R[e] = jnp.zeros(R.shape[1:], jnp.float32)
    R[e, 0:top, :] = IDS[...].astype(jnp.float32)
    R[e, top : 2 * top, :] = RW[...]
    pl.semaphore_wait(barrier, 6 + inner.astype(jnp.int32))

    def send(kind, src, dst, recv, target, when=None):
        c = pltpu.make_async_remote_copy(
            src_ref=src, dst_ref=dst, send_sem=ssem.at[kind], recv_sem=recv,
            device_id=target, device_id_type=MESH,
        )
        if when is None:
            c.start()
        else:
            pl.when(when)(c.start)

    def arrived(ref, sem):
        pltpu.make_async_remote_copy(
            src_ref=ref, dst_ref=ref, send_sem=ssem.at[0], recv_sem=sem,
            device_id={"seq": oq}, device_id_type=MESH,
        ).wait_recv()

    def sent(kind, ref):
        pltpu.make_async_remote_copy(
            src_ref=ref, dst_ref=ref, send_sem=ssem.at[kind], recv_sem=ssem.at[kind],
            device_id={"seq": oq}, device_id_type=MESH,
        ).wait_send()

    lot = block_rows // 2

    def chunk(group, part, k, h):
        return T.at[k, pl.ds(pl.multiple_of(group * rows + part * block_rows + h * lot, lot), lot)]

    def slot(group, part, k, h):
        return rsem.at[((group * 2 + part) * S + k) * 2 + h]

    def push(kind, group, part, k, target, when=None, lots=(0, 1)):
        for h in lots:
            c = chunk(group, part, k, h)
            send(kind, c, c, slot(group, part, k, h), target, when)

    def take(group, part, k, lots=(0, 1)):
        for h in lots:
            arrived(chunk(group, part, k, h), slot(group, part, k, h))

    for target in (to_core, {"expert": oyc}, to_y):
        send(3, R.at[e], R.at[e], rrsem.at[e], target)
    push(0, e, 1 - side, s, to_core)
    push(0, e, side, s, to_core)

    def nearest(n, lots=(0, 1)):
        push(2, near + n, side, s, up, s != S - 1, lots)
        push(2, near + n, side, s, down, s != 0, lots)

    for n in (0, 1):

        @pl.when(side != n)
        def _():
            take(near + n, side, s)

        push(2, near + n, side, s, skip)
        if n == 0:
            nearest(n)
        push(1, near + n, side, s, to_y)

    me = e.astype(jnp.float32)
    before = (
        lax.broadcasted_iota(jnp.int32, (rows, rows), 0) < lax.broadcasted_iota(jnp.int32, (rows, rows), 1)
    ).astype(jnp.float32).astype(jnp.bfloat16)

    def dispatch(g):
        table = R[g]
        named = jnp.zeros((1, rows), jnp.float32)
        weight = jnp.zeros((1, rows), jnp.float32)
        for n in range(top):
            hit = (table[n : n + 1, :] == me).astype(jnp.float32)
            named = named + hit
            weight = weight + hit * table[top + n : top + n + 1, :]
        rank = jnp.dot(
            jnp.broadcast_to(named, (8, rows)).astype(jnp.bfloat16), before, preferred_element_type=jnp.float32
        )[0:1, :]
        place = lax.broadcasted_iota(jnp.int32, (cap, rows), 0).astype(jnp.float32)
        match = jnp.where(place == rank, 1.0, 0.0) * named
        DISP[g] = match.astype(jnp.bfloat16)
        WR[g] = jnp.broadcast_to(jnp.sum(match * weight, axis=1, keepdims=True), (cap, WR.shape[2]))

    def z_in(n, i, when=None, lots=(0, 1)):
        if when is not None:
            pl.when(when)(functools.partial(z_in, n, i, None, lots))
            return
        for h in lots:
            take(near + n, side, sec[i], (h,))
            if i == 1:
                push(2, near + n, side, sec[i], {"section": out_sec}, inner, (h,))
            push(1, near + n, side, sec[i], to_y, None, (h,))
            push(0, near + n, side, sec[i], to_core, None, (h,))

    def y_in(n, i, lots=(0, 1)):
        for h in lots:
            take(far + n, side, sec[i], (h,))
            push(0, far + n, side, sec[i], to_core, None, (h,))

    groups = [near, far, near + 1, far + 1]
    loaded = set()

    def span(g):
        return pl.ds(pl.multiple_of(g * cap, cap), cap)

    def block(m, i):
        g, k = groups[m], sec[i]
        if m % 2 == 0 and i == 0:

            @pl.when(side != m // 2)
            def _():
                take(g, 1 - side, k)
        else:
            take(g, 1 - side, k)
        if i not in loaded:
            loaded.add(i)
            for c in loads[i]:
                c.wait()
        lines = pl.ds(pl.multiple_of(g * rows, rows), rows)
        for W, A in ((WG, G), (WU, U)):
            v = jnp.dot(T[k, lines, :], W[bands[i], :], preferred_element_type=jnp.float32)
            if i == 0:
                A[m] = v
            else:
                A[m] = A[m] + v

    def hidden_out(m):
        a = G[m]
        h = (a / (1.0 + jnp.exp(-a)) * U[m]).astype(jnp.bfloat16)
        HO[m] = jnp.dot(DISP[groups[m]], h, preferred_element_type=jnp.float32).astype(jnp.bfloat16)
        send(4, HO.at[m], HX.at[m], hsem.at[m], to_x)

    own_units = pl.ds(pl.multiple_of(q * units, units), units)
    other_units = pl.ds(pl.multiple_of(oq * units, units), units)
    part = outs // 2
    chunks = YS.shape[1]
    width = part // chunks
    mine, theirs = (pl.ds(pl.multiple_of(h * part, part), part) for h in (side, 1 - side))

    def ahead(m):
        if m == 1:
            down_load.wait()
        PO[m] = jnp.dot(HO[m], WD[own_units, :], preferred_element_type=jnp.float32)

    def half(m, cols):
        g = groups[m]
        v = PO[m, :, cols] + jnp.dot(HX[m], WD[other_units, cols], preferred_element_type=jnp.float32)
        v = (v * WR[g][:, 0:1]).astype(jnp.bfloat16)
        return lax.dot_general(DISP[g], v, (((0,), (0,)), ((), ())), preferred_element_type=jnp.float32)

    def to_partner(m):
        CS[m] = half(m, theirs).astype(jnp.bfloat16)
        send(5, CS.at[m], CR.at[m], csem.at[m], to_core)

    def keep(m):
        ACC[m] = half(m, mine)
        arrived(CR.at[m], csem.at[m])

    def piece(m, n):
        cols = slice(n * width, (n + 1) * width)
        return ACC[m, :, cols] + CR[m, :, cols].astype(jnp.float32)

    def to_neighbour(b):
        for n in range(chunks):
            YS[b, n] = piece(2 * b + 1, n).astype(jnp.bfloat16)
            send(6, YS.at[b, n], YR.at[b, n], ysem.at[b, n], to_y)

    def first(a, n):
        arrived(YR.at[a, n], ysem.at[a, n])
        total = piece(2 * a, n) + YR[a, n].astype(jnp.float32)

        @pl.when(outer)
        def _():
            ZS[a, n] = total.astype(jnp.bfloat16)

        @pl.when(inner)
        def _():
            PF[a, n] = total

        send(7, ZS.at[a, n], ZR.at[a, n], zsem.at[a, n], {"section": in_sec}, outer)

    def second(a, n):
        @pl.when(inner)
        def _():
            arrived(ZR.at[a, n], zsem.at[a, n])
            ZS[a, n] = (PF[a, n] + ZR[a, n].astype(jnp.float32)).astype(jnp.bfloat16)

        send(7, ZS.at[a, n], ZX.at[a, n], xsem.at[a, n], {"section": cross}, inner)

    def drain(h):
        for n in range(chunks):
            cols = pl.ds(pl.multiple_of(h * part + n * width, width), width)
            out_hbm[:, cols] = OUT[h, n]

    def third(a, n):
        @pl.when(inner)
        def _():
            arrived(ZX.at[a, n], xsem.at[a, n])
            total = (ZS[a, n].astype(jnp.float32) + ZX[a, n].astype(jnp.float32)).astype(jnp.bfloat16)
            ZO[a, n] = total

            @pl.when(side == a)
            def _():
                OUT[side, n] = total

        send(8, ZO.at[a, n], OUT.at[side, n], osem.at[side], {"section": out_sec, "expert": near + a}, inner)
        send(9, ZO.at[a, n], OUT.at[side, n], osem.at[side], to_core, inner & (side != a))

    def hidden_in(m):
        arrived(HX.at[m], hsem.at[m])

    block(0, 0)
    for g in (core, oy, oyc):
        arrived(R.at[g], rrsem.at[g])
    block(2, 0)
    dispatch(near)
    dispatch(far)
    dispatch(near + 1)
    dispatch(far + 1)
    y_in(0, 0)
    z_in(0, 1, None, (0,))
    z_in(0, 2, None, (0,))
    z_in(0, 1, None, (1,))
    nearest(1)
    z_in(0, 2, None, (1,))
    block(1, 0)
    y_in(1, 0)
    block(0, 1)
    z_in(0, 3, None, (0,))
    block(0, 2)
    z_in(0, 3, None, (1,))
    z_in(1, 1, inner)
    y_in(0, 1)
    block(3, 0)
    block(0, 3)
    hidden_out(0)
    y_in(0, 2)
    block(1, 1)
    z_in(1, 1, outer, (0,))
    z_in(1, 2, None, (0,))
    y_in(0, 3, (0,))
    block(1, 2)
    z_in(1, 1, outer, (1,))
    z_in(1, 2, None, (1,))
    y_in(0, 3, (1,))
    block(2, 1)
    block(1, 3)
    hidden_out(1)
    z_in(1, 3, None, (0,))
    block(2, 2)
    z_in(1, 3, None, (1,))
    ahead(1)
    block(2, 3)
    hidden_out(2)
    y_in(1, 1)
    ahead(0)
    block(3, 1)
    y_in(1, 2)
    hidden_in(0)
    to_partner(0)
    block(3, 2)
    y_in(1, 3)
    hidden_in(1)
    to_partner(1)
    block(3, 3)
    hidden_out(3)
    keep(1)
    to_neighbour(0)
    keep(0)
    ahead(2)
    ahead(3)
    hidden_in(2)
    to_partner(2)
    keep(2)
    cut = chunks // 2
    for n in range(cut):
        first(0, n)
    hidden_in(3)
    to_partner(3)
    for n in range(cut, cut + 2):
        first(0, n)
    keep(3)
    to_neighbour(1)
    for n in range(cut + 2, chunks):
        first(0, n)
    for n in range(chunks):
        second(0, n)
    for n in range(chunks + 2 * cut):
        if n < chunks:
            third(0, n)
            first(1, n)
        if cut <= n < chunks + cut:
            second(1, n - cut)
        if n >= 2 * cut:
            third(1, n - 2 * cut)

    @pl.when(outer)
    def _():
        arrived(OUT.at[side], osem.at[side])

    drain(side)
    arrived(OUT.at[1 - side], osem.at[1 - side])
    drain(1 - side)
    sent(0, T.at[0:2])
    sent(1, T.at[0])
    sent(3, R.at[0:3])
    sent(4, HO)
    sent(5, CS)
    sent(6, YS)
    sent(7, ZS)

    @pl.when(outer)
    def _():
        sent(2, T.at[0, 0 : 2 * rows])

    @pl.when(inner)
    def _():
        sent(2, T.at[0])
        sent(8, ZO)
        sent(9, ZO.at[0])


def fused(tokens, route_ids, route_weights, gate_weight, up_weight, down_weight):
    S, E = lax.axis_size("section"), lax.axis_size("expert")
    rows, feat = tokens.shape
    top = route_ids.shape[1]
    cap = 3 * rows * top // (2 * E)
    units, outs = gate_weight.shape[2], down_weight.shape[2]
    table_rows = -(-2 * top // 8) * 8
    bf, f32 = jnp.bfloat16, jnp.float32
    dma = pltpu.SemaphoreType.DMA
    sends = 10
    part, chunks = outs // 2, outs // 256
    grid = (2, chunks, rows, part // chunks)
    return pl.pallas_call(
        functools.partial(kernel, S, E, top, cap),
        out_shape=pltpu.VMEM((rows, outs), bf),
        in_specs=[pl.BlockSpec(memory_space=pl.ANY)] * 6,
        out_specs=pl.BlockSpec(memory_space=pltpu.VMEM),
        scratch_shapes=[
            pltpu.VMEM((S, E * rows, feat), bf),
            pltpu.VMEM((top, rows), jnp.int32),
            pltpu.VMEM((top, rows), f32),
            pltpu.VMEM((E, table_rows, rows), f32),
            pltpu.VMEM((S * feat, units), bf),
            pltpu.VMEM((S * feat, units), bf),
            pltpu.VMEM(down_weight.shape[1:], bf),
            pltpu.VMEM((E, cap, rows), bf),
            pltpu.VMEM((E, cap, 128), f32),
            pltpu.VMEM((E, rows, units), f32),
            pltpu.VMEM((E, rows, units), f32),
            pltpu.VMEM((E, cap, units), bf),
            pltpu.VMEM((E, cap, units), bf),
            pltpu.VMEM((E, cap, outs), f32),
            pltpu.VMEM((4, rows, part), bf),
            pltpu.VMEM((4, rows, part), bf),
            pltpu.VMEM((4, rows, part), f32),
            pltpu.VMEM(grid, bf),
            pltpu.VMEM(grid, bf),
            pltpu.VMEM(grid, f32),
            pltpu.VMEM(grid, bf),
            pltpu.VMEM(grid, bf),
            pltpu.VMEM(grid, bf),
            pltpu.VMEM(grid, bf),
            pltpu.VMEM(grid, bf),
            dma((2 * S + 1,)),
            dma((3,)),
            dma((sends,)),
            dma((4 * E * S,)),
            dma((E,)),
            dma((4,)),
            dma((4,)),
            dma((2, chunks)),
            dma((2, chunks)),
            dma((2, chunks)),
            dma((2,)),
            dma((1,)),
        ],
        compiler_params=pltpu.CompilerParams(
            collective_id=0, has_side_effects=True, vmem_limit_bytes=60 * 1024 * 1024
        ),
    )(tokens, route_ids.T, route_weights.T, gate_weight, up_weight, down_weight)


def shards(tokens, route_ids, route_weights, gate_weight, up_weight, down_weight):
    args = (tokens, route_ids, route_weights, gate_weight, up_weight, down_weight)
    pairs = lax.axis_size("expert") == 2 * 2 and lax.axis_size("seq") == 2
    if pairs and lax.axis_size("section") == 4:
        return fused(*args)
    return plain(*args)


def solution(mesh):
    in_specs = (
        P("expert", "section"),
        P("expert", None),
        P("expert", None),
        P("expert", None, ("section", "seq")),
        P("expert", None, ("section", "seq")),
        P("expert", "section", "seq"),
    )
    out_specs = P("expert", "seq")
    return jax.shard_map(shards, mesh=mesh, in_specs=in_specs, out_specs=out_specs, check_vma=False)
```
